16 devices in a mesh: dp: 4 (over y, z, core), tp: 4 (over x).
Axes of the slice: x: 4, y: 2, z: 1, core: 2. Of those that a mesh axis runs over, the one named last changes fastest.
The devices are a block of a 4x4x8 slice.
Arguments:
- x: bfloat16 [16384, 1024], P(('dp', 'tp')), parts along dimension 0
- gain: bfloat16 [1024], replicated
- wq: bfloat16 [1024, 4096], P(None, 'tp')
- wk: bfloat16 [1024, 4096], P(None, 'tp')
- wv: bfloat16 [1024, 4096], P(None, 'tp')
- wo: bfloat16 [4096, 1024], P('tp')
Outputs:
- output: bfloat16 [16384, 1024], P(('dp', 'tp')), parts along dimension 0
There are 4 independent parts. The reference program is written for one: setup_inputs(seed, part) draws one part's arguments, and reference() takes and returns one part's arrays. A program takes and returns all parts, laid end to end along the dimension named above; an argument that names none is the same for every part.
All inputs are finite; a program needn't handle non-finite values.
Results may differ from the reference program's by a relative error of at most 0.012.
Values are sent between devices in bfloat16 or wider.
A program may use at most 768 MiB of HBM per device.

```python
import jax
import jax.numpy as jnp
from jax import lax

ROWS = 4096
D = 1024
HEADS = 32
KV_HEADS = 32
HEAD = 128
THETA = 10000


def setup_inputs(seed: int = 0, part: int = 0) -> dict:
    kx, kn, kq, kk, kv, ko = jax.random.split(jax.random.key(seed), 6)

    def weights(key, rows, columns):
        return jax.random.normal(key, (rows, columns), jnp.float32) * rows**-0.5

    drawn = {
        "x": jax.random.normal(jax.random.fold_in(kx, part), (ROWS, D), jnp.float32),
        "gain": 1 + 0.1 * jax.random.normal(kn, (D,), jnp.float32),
        "wq": 2 * weights(kq, D, HEADS * HEAD),
        "wk": 2 * weights(kk, D, KV_HEADS * HEAD),
        "wv": 4 * weights(kv, D, KV_HEADS * HEAD),
        "wo": weights(ko, HEADS * HEAD, D),
    }
    return {k: v.astype(jnp.bfloat16) for k, v in drawn.items()}


def normed(x, gain):
    wide = x.astype(jnp.float32)
    scale = lax.rsqrt(jnp.mean(wide * wide, -1, keepdims=True) + 1e-6)
    return (wide * scale * gain.astype(jnp.float32)).astype(jnp.bfloat16)


def turned(t, place, theta):
    half = t.shape[-1] // 2
    angle = place.astype(jnp.float32)[:, None] * theta ** (-jnp.arange(half, dtype=jnp.float32) / half)
    cos, sin = jnp.cos(angle)[:, None], jnp.sin(angle)[:, None]
    a, b = t[..., :half].astype(jnp.float32), t[..., half:].astype(jnp.float32)
    return jnp.concatenate([a * cos - b * sin, b * cos + a * sin], -1).astype(jnp.bfloat16)


def matmul(a, w):
    return jnp.dot(a, w, preferred_element_type=jnp.float32).astype(jnp.bfloat16)


def einsum(form, a, b):
    return jnp.einsum(form, a.astype(jnp.float32), b.astype(jnp.float32))


def attention(q, k, v):
    scores = einsum("tgsd,ugd->gstu", q, k) * q.shape[-1] ** -0.5
    token = jnp.arange(q.shape[0])
    scores = jnp.where(token[:, None] >= token, scores, -jnp.inf)
    weights = jax.nn.softmax(scores, -1).astype(jnp.bfloat16)
    return einsum("gstu,ugd->tgsd", weights, v).astype(jnp.bfloat16)


def reference(x, gain, wq, wk, wv, wo):
    a, place = normed(x, gain), jnp.arange(ROWS)
    q = turned(matmul(a, wq).reshape(ROWS, HEADS, HEAD), place, THETA).reshape(ROWS, KV_HEADS, -1, HEAD)
    k = turned(matmul(a, wk).reshape(ROWS, KV_HEADS, HEAD), place, THETA)
    v = matmul(a, wv).reshape(ROWS, KV_HEADS, HEAD)
    seen = attention(q, k, v).reshape(ROWS, HEADS * HEAD)
    return (x.astype(jnp.float32) + jnp.dot(seen, wo, preferred_element_type=jnp.float32)).astype(jnp.bfloat16)
```

```python
import functools

import jax
import jax.numpy as jnp
import numpy as np
from jax import lax
from jax.experimental import pallas as pl
from jax.experimental.pallas import tpu as pltpu
from jax.sharding import PartitionSpec as P

HEAD = 128
THETA = 10000
NEG = -1e30
HIDDEN = 2 * NEG
LOG2E = 1.4426950408889634
RING = 4
PER = 4
KB = 512
MESH = pl.DeviceIdType.MESH
VMEM = 67043328


def _dot(a, b, ca, cb):
    return lax.dot_general(a, b, (((ca,), (cb,)), ((), ())), preferred_element_type=jnp.float32)


def _kernel(x_hbm, gain_ref, bc_ref, bs_ref, gc_ref, gs_ref, wq_hbm, wk_hbm, wv_hbm, wo_hbm, y_hbm, xg_hbm, full_hbm,
            q_s, k_s, vt_s, acc_s, top_s, w_s, wo_s, x_s, xn_s, cos_s, sin_s, seen_s, term_s, send_s, half_s, got_s,
            w_sem, x_sem, got_sem, y_sem, ag_send, ag_recv, rs_send, rs_recv):
    ch = x_s.shape[1]
    heads = q_s.shape[1] // HEAD
    wide = 2 * HEAD
    me = lax.axis_index("tp")
    right, left, opp = lax.rem(me + 1, RING), lax.rem(me + 3, RING), lax.rem(me + 2, RING)
    e = HEAD**-0.5 * LOG2E

    weights = [pltpu.make_async_copy(w, w_s.at[i], w_sem.at[i]) for i, w in enumerate((wq_hbm, wk_hbm, wv_hbm))]
    weights.append(pltpu.make_async_copy(wo_hbm, wo_s, w_sem.at[3]))
    for w in weights:
        w.start()

    barrier = pltpu.get_barrier_semaphore()
    for side in (left, right):
        pl.semaphore_signal(barrier, inc=1, device_id={"tp": side}, device_id_type=MESH)
    pl.semaphore_wait(barrier, 2)

    def rows(c):
        return pl.ds(pl.multiple_of(c * ch, ch), ch)

    def gather(side, i, src, slot, c):
        n = side * 6 + i
        return pltpu.make_async_remote_copy(src_ref=src, dst_ref=xg_hbm.at[slot, rows(c)], send_sem=ag_send.at[n], recv_sem=ag_recv.at[n],
                                            device_id={"tp": (right, left)[side]}, device_id_type=MESH)

    for i in range(PER):
        c = (i + 2) % PER
        gather(0, i, x_hbm.at[rows(i)], 0, i).start()
        gather(1, i, x_hbm.at[rows(c)], 1, c).start()

    def clear(slot):
        acc_s[slot] = jnp.zeros(acc_s.shape[1:], jnp.float32)
        top_s[slot] = jnp.full(top_s.shape[1:], NEG, jnp.float32)

    def state(b, c):
        rel = lax.rem(b - me + RING, RING)
        return jnp.where(rel == 2, 3 * PER, jnp.where(rel == 3, 2 * PER, rel * PER) + c)

    def project(b, c, at):
        g = b * PER + c
        wide_x = x_s[at].astype(jnp.float32)
        scale = lax.rsqrt(jnp.mean(wide_x * wide_x, -1, keepdims=True) + 1e-6)
        xn_s[...] = (wide_x * scale * gain_ref[...].astype(jnp.float32)).astype(jnp.bfloat16)
        gc, gs = gc_ref[pl.ds(g, 1), :], gs_ref[pl.ds(g, 1), :]
        cos_s[...] = gc * bc_ref[...] - gs * bs_ref[...]
        sin = gs * bc_ref[...] + gc * bs_ref[...]
        sin_s[...] = jnp.where(lax.broadcasted_iota(jnp.int32, sin.shape, 1) < HEAD // 2, -sin, sin)
        for n in range(0, heads * HEAD, wide):
            for i, out in ((0, q_s), (1, k_s)):
                t = _dot(xn_s[...], w_s[i, :, n : n + wide], 1, 0).astype(jnp.bfloat16).astype(jnp.float32)
                for h in range(0, wide, HEAD):
                    a = t[:, h : h + HEAD]
                    out[rows(g), n + h : n + h + HEAD] = (a * cos_s[...] + pltpu.roll(a, HEAD // 2, 1) * sin_s[...]).astype(jnp.bfloat16)
            v = _dot(xn_s[...], w_s[2, :, n : n + wide], 1, 0).astype(jnp.bfloat16)
            vt_s[n : n + wide, rows(g)] = v.T

    def block(g, slot, first, bk, masked):
        keys = pl.ds(pl.multiple_of(first, bk), bk)
        cols = [slice(h * HEAD, (h + 1) * HEAD) for h in range(heads)]
        scores = [_dot(k_s[keys, c], q_s[rows(g), c], 1, 1) for c in cols]
        ok = None
        if masked:
            shape = (bk, ch)
            gap = lax.broadcasted_iota(jnp.int32, shape, 1) - lax.broadcasted_iota(jnp.int32, shape, 0)
            ok = gap >= first - g * ch
        ones = jnp.ones((8, bk), jnp.bfloat16)
        probs, keeps = [], []
        for h, s in enumerate(scores):
            if masked:
                s = jnp.where(ok, s, HIDDEN)
            old = top_s[slot, h : h + 1, :]
            top = jnp.maximum(old, s.max(axis=0, keepdims=True))
            top_s[slot, h : h + 1, :] = top
            probs.append(jnp.exp2((s - top) * e).astype(jnp.bfloat16))
            keeps.append(jnp.exp2((old - top) * e))
        for h, (p, keep) in enumerate(zip(probs, keeps)):
            values = jnp.concatenate([vt_s[cols[h], keys], ones], axis=0)
            acc_s[slot, h] = acc_s[slot, h] * keep + _dot(values, p, 1, 0)

    def whole(g, slot, first, count):
        lax.fori_loop(0, count, lambda j, _: block(g, slot, first + j * KB, KB, False), None)

    def diagonal(g, slot, b, c, count):
        at = (b * PER + 2 * (c // 2)) * ch
        lax.fori_loop(0, count, lambda j, _: block(g, slot, at + j * ch, ch, True), None)

    def round_(r, _):
        mine, far = r < 2, r >= 6
        i = jnp.where(mine, 0, jnp.where(far, r - 6, r - 2))
        n = jnp.where(far, i + 4, i)
        ca, cb = jnp.where(mine, 2 * r, i), jnp.where(mine, 2 * r + 1, lax.rem(i + 2, PER))
        ba = jnp.where(mine, me, jnp.where(far, opp, left))
        bb = jnp.where(mine, me, jnp.where(far, opp, right))

        @pl.when(mine)
        def _():
            pltpu.make_async_copy(x_hbm.at[rows(ca)], x_s.at[0], x_sem.at[0]).start()
            pltpu.make_async_copy(x_hbm.at[rows(cb)], x_s.at[1], x_sem.at[1]).start()

        @pl.when(r >= 2)
        def _():
            sa, sb = jnp.where(far, 2, 0), jnp.where(far, 2, 1)
            gather(0, n, xg_hbm.at[0, rows(ca)], sa, ca).wait_recv()
            gather(1, n, xg_hbm.at[1, rows(cb)], sb, cb).wait_recv()

            @pl.when(r < 4)
            def _():
                gather(0, i + 4, xg_hbm.at[0, rows(ca)], 2, ca).start()
                gather(1, i + 4, xg_hbm.at[1, rows(cb)], 2, cb).start()

            pltpu.make_async_copy(xg_hbm.at[sa, rows(ca)], x_s.at[0], x_sem.at[0]).start()
            pltpu.make_async_copy(xg_hbm.at[sb, rows(cb)], x_s.at[1], x_sem.at[1]).start()

        @pl.when(r == 0)
        def _():
            for w in weights:
                w.wait()

        def chunk(j, _):
            pltpu.make_async_copy(x_hbm.at[rows(0)], x_s.at[j], x_sem.at[j]).wait()
            b, c = jnp.where(j == 0, ba, bb), jnp.where(j == 0, ca, cb)

            @pl.when(jnp.logical_not(far))
            def _():
                clear(state(b, c))

            project(b, c, j)

        lax.fori_loop(0, 2, chunk, None)

        @pl.when(r == 1)
        def _():
            def own(c, _):
                g = me * PER + c
                whole(g, c, me * PER * ch, c // 2)
                diagonal(g, c, me, c, 1 + c % 2)

            lax.fori_loop(0, PER, own, None)

        @pl.when((r == 3) | (r == 5))
        def _():
            def pair(n, _):
                j, from_left = n % 4, n < 4
                other = jnp.where(from_left, left, right)
                half = jnp.where((r == 3) == from_left, 0, 1)
                later = me > other
                b = jnp.where(later, me, other)
                c = jnp.where(later, j, 2 * half + j // 2)
                kh = jnp.where(later, 2 * other + half, 2 * me + j % 2)
                block(b * PER + c, state(b, c), kh * KB, KB, False)

            lax.fori_loop(0, 8, pair, None)

    lax.fori_loop(0, 8, round_, None)

    def halves(side, s):
        part = pl.ds(side * (ch // 2), ch // 2)
        n = side * PER + s
        return pltpu.make_async_remote_copy(src_ref=send_s.at[0, lax.rem(s, 2), part], dst_ref=half_s.at[side, s], send_sem=rs_send.at[n],
                                            recv_sem=rs_recv.at[n], device_id={"tp": (right, left)[side]}, device_id_type=MESH)

    def fulls(side, s):
        n = (2 + side) * PER + s
        return pltpu.make_async_remote_copy(src_ref=send_s.at[1 + side, lax.rem(s, 2)], dst_ref=full_hbm.at[side, s], send_sem=rs_send.at[n],
                                            recv_sem=rs_recv.at[n], device_id={"tp": (right, left)[side]}, device_id_type=MESH)

    def item(n, _):
        m = jnp.where(n >= 10, n, n - 1)
        kind = jnp.where(n == 0, 0, jnp.where(n >= 12, 3, m % 3))
        s = jnp.where(n == 0, 0, jnp.where(n >= 12, n - 12, m // 3 + jnp.where(m % 3 == 0, 1, 0)))
        b = jnp.where(kind == 0, opp, jnp.where(kind == 1, right, jnp.where(kind == 2, left, me)))
        g, slot = b * PER + s, state(b, s)

        @pl.when(kind == 0)
        def _():
            clear(slot)

        def over(kb, _):
            done = ((b == me) & (kb != opp)) | ((kb == me) & (b != opp))
            count = jnp.where(kb == b, jnp.where(b == me, 0, s // 2), jnp.where(done, 0, 2))
            whole(g, slot, kb * PER * ch, count)

        lax.fori_loop(0, b + 1, over, None)
        diagonal(g, slot, b, s, jnp.where(b == me, 0, 1 + s % 2))

        for h in range(heads):
            total = acc_s[slot, h, HEAD : HEAD + 1, :]
            seen_s[:, h * HEAD : (h + 1) * HEAD] = (acc_s[slot, h, :HEAD, :] * (1 / total)).astype(jnp.bfloat16).T
        for j in range(0, term_s.shape[1], wide):
            term_s[:, j : j + wide] = _dot(seen_s[...], wo_s[:, j : j + wide], 1, 0)

        @pl.when(kind == 0)
        def _():
            @pl.when(s >= 2)
            def _():
                halves(0, s - 2).wait_send()
                halves(1, s - 2).wait_send()

            send_s[0, lax.rem(s, 2)] = term_s[...].astype(jnp.bfloat16)
            halves(0, s).start()
            halves(1, s).start()

        for side in range(2):

            @pl.when(kind == 1 + side)
            def _(side=side):
                @pl.when(s >= 2)
                def _():
                    fulls(side, s - 2).wait_send()

                halves(side, s).wait_recv()
                mid = ch // 2
                near, rest = slice(side * mid, (side + 1) * mid), slice((1 - side) * mid, (2 - side) * mid)
                to = lax.rem(s, 2)
                send_s[1 + side, to, rest] = term_s[rest].astype(jnp.bfloat16)
                send_s[1 + side, to, near] = (term_s[near] + half_s[side, s].astype(jnp.float32)).astype(jnp.bfloat16)
                fulls(side, s).start()

        @pl.when(kind == 3)
        def _():
            token = pltpu.make_async_copy(x_hbm.at[rows(s)], x_s.at[0], x_sem.at[0])
            token.start()
            come = []
            for side in range(2):
                fulls(side, s).wait_recv()
                come.append(pltpu.make_async_copy(full_hbm.at[side, s], got_s.at[side], got_sem.at[side]))
                come[side].start()
            token.wait()
            for one in come:
                one.wait()
            total = term_s[...] + got_s[0].astype(jnp.float32) + got_s[1].astype(jnp.float32)
            x_s[1] = (x_s[0].astype(jnp.float32) + total).astype(jnp.bfloat16)
            done = pltpu.make_async_copy(x_s.at[1], y_hbm.at[rows(s)], y_sem)
            done.start()
            done.wait()

    lax.fori_loop(0, 4 * PER, item, None)

    for side in range(2):
        for i in range(6):
            gather(side, i, x_hbm.at[rows(0)], 0, 0).wait_send()
        for s in (PER - 2, PER - 1):
            halves(side, s).wait_send()
            fulls(side, s).wait_send()


def solution(mesh):
    def step(x, gain, wq, wk, wv, wo):
        t, d = x.shape
        ch, columns = t // PER, wq.shape[1]
        heads, every = columns // HEAD, t * RING
        rate = np.float64(THETA) ** (-np.arange(HEAD // 2) / (HEAD // 2))
        rate = np.concatenate([rate, rate])
        base, far = np.arange(ch)[:, None] * rate, (np.arange(every // ch) * ch)[:, None] * rate
        tables = [jnp.asarray(f(a), jnp.float32) for a in (base, far) for f in (np.cos, np.sin)]
        hbm, vmem = pl.BlockSpec(memory_space=pl.ANY), pl.BlockSpec(memory_space=pltpu.VMEM)
        bf, f32 = jnp.bfloat16, jnp.float32
        y, _, _ = pl.pallas_call(
            _kernel,
            out_shape=[jax.ShapeDtypeStruct((t, d), bf), jax.ShapeDtypeStruct((3, t, d), bf), jax.ShapeDtypeStruct((2, PER, ch, d), bf)],
            in_specs=[hbm] + [vmem] * 5 + [hbm] * 4,
            out_specs=[hbm] * 3,
            scratch_shapes=[
                pltpu.VMEM((every, columns), bf),
                pltpu.VMEM((every, columns), bf),
                pltpu.VMEM((columns, every), bf),
                pltpu.VMEM((3 * PER + 1, heads, HEAD + 8, ch), f32),
                pltpu.VMEM((3 * PER + 1, heads, ch), f32),
                pltpu.VMEM((3, d, columns), bf),
                pltpu.VMEM((columns, d), bf),
                pltpu.VMEM((2, ch, d), bf),
                pltpu.VMEM((ch, d), bf),
                pltpu.VMEM((ch, HEAD), f32),
                pltpu.VMEM((ch, HEAD), f32),
                pltpu.VMEM((ch, columns), bf),
                pltpu.VMEM((ch, d), f32),
                pltpu.VMEM((3, 2, ch, d), bf),
                pltpu.VMEM((2, PER, ch // 2, d), bf),
                pltpu.VMEM((2, ch, d), bf),
                pltpu.SemaphoreType.DMA((4,)),
                pltpu.SemaphoreType.DMA((2,)),
                pltpu.SemaphoreType.DMA((2,)),
                pltpu.SemaphoreType.DMA,
                pltpu.SemaphoreType.DMA((12,)),
                pltpu.SemaphoreType.DMA((12,)),
                pltpu.SemaphoreType.DMA((4 * PER,)),
                pltpu.SemaphoreType.DMA((4 * PER,)),
            ],
            compiler_params=pltpu.CompilerParams(collective_id=0, has_side_effects=True, vmem_limit_bytes=VMEM),
        )(x, gain[None], *tables[:2], *tables[2:], wq, wk, wv, wo)
        return y

    tokens, columns = P(("dp", "tp"), None), P(None, "tp")
    return jax.shard_map(
        step,
        mesh=mesh,
        in_specs=(tokens, P(None), columns, columns, columns, P("tp", None)),
        out_specs=tokens,
        check_vma=False,
    )
```

```python
import functools

import jax
import jax.numpy as jnp
import numpy as np
from jax import lax
from jax.experimental import pallas as pl
from jax.experimental.pallas import tpu as pltpu
from jax.sharding import PartitionSpec as P

HEAD = 128
THETA = 10000
NEG = -1e30
HIDDEN = 2 * NEG
LOG2E = 1.4426950408889634
RING = 4
PER = 4
KB = 512
MESH = pl.DeviceIdType.MESH
VMEM = 67043328


def _dot(a, b, ca, cb):
    return lax.dot_general(a, b, (((ca,), (cb,)), ((), ())), preferred_element_type=jnp.float32)


def _kernel(x_hbm, gain_ref, bc_ref, bs_ref, gc_ref, gs_ref, wq_hbm, wk_hbm, wv_hbm, wo_hbm, y_hbm, xg_hbm, full_hbm,
            q_s, k_s, vt_s, acc_s, top_s, s_s, high_s, w_s, x_s, xn_s, cos_s, sin_s, seen_s, term_s, send_s, half_s, got_s,
            w_sem, x_sem, got_sem, y_sem, ag_send, ag_recv, rs_send, rs_recv):
    ch = x_s.shape[1]
    heads = q_s.shape[1] // HEAD
    wide = 2 * HEAD
    me = lax.axis_index("tp")
    right, left, opp = lax.rem(me + 1, RING), lax.rem(me + 3, RING), lax.rem(me + 2, RING)
    e = HEAD**-0.5 * LOG2E

    weights = [pltpu.make_async_copy(w, w_s.at[i], w_sem.at[i]) for i, w in enumerate((wq_hbm, wk_hbm, wv_hbm))]
    last = pltpu.make_async_copy(wo_hbm, w_s.at[0], w_sem.at[3])
    for w in weights:
        w.start()

    barrier = pltpu.get_barrier_semaphore()
    for side in (left, right):
        pl.semaphore_signal(barrier, inc=1, device_id={"tp": side}, device_id_type=MESH)
    pl.semaphore_wait(barrier, 2)

    def rows(c):
        return pl.ds(pl.multiple_of(c * ch, ch), ch)

    def gather(side, i, src, slot, c):
        n = side * 6 + i
        return pltpu.make_async_remote_copy(src_ref=src, dst_ref=xg_hbm.at[slot, rows(c)], send_sem=ag_send.at[n], recv_sem=ag_recv.at[n],
                                            device_id={"tp": (right, left)[side]}, device_id_type=MESH)

    for i in range(PER):
        c = (i + 2) % PER
        gather(0, i, x_hbm.at[rows(i)], 0, i).start()
        gather(1, i, x_hbm.at[rows(c)], 1, c).start()

    def clear(slot):
        acc_s[slot] = jnp.zeros(acc_s.shape[1:], jnp.float32)
        top_s[slot] = jnp.full(top_s.shape[1:], NEG, jnp.float32)

    def state(b, c):
        rel = lax.rem(b - me + RING, RING)
        return jnp.where(rel == 2, 3 * PER, jnp.where(rel == 3, 2 * PER, rel * PER) + c)

    def project(b, c, at):
        g = b * PER + c
        wide_x = x_s[at].astype(jnp.float32)
        scale = lax.rsqrt(jnp.mean(wide_x * wide_x, -1, keepdims=True) + 1e-6)
        xn_s[...] = (wide_x * scale * gain_ref[...].astype(jnp.float32)).astype(jnp.bfloat16)
        gc, gs = gc_ref[pl.ds(g, 1), :], gs_ref[pl.ds(g, 1), :]
        cos_s[...] = gc * bc_ref[...] - gs * bs_ref[...]
        sin = gs * bc_ref[...] + gc * bs_ref[...]
        sin_s[...] = jnp.where(lax.broadcasted_iota(jnp.int32, sin.shape, 1) < HEAD // 2, -sin, sin)
        for n in range(0, heads * HEAD, wide):
            for i, out in ((0, q_s), (1, k_s)):
                t = _dot(xn_s[...], w_s[i, :, n : n + wide], 1, 0).astype(jnp.bfloat16).astype(jnp.float32)
                for h in range(0, wide, HEAD):
                    a = t[:, h : h + HEAD]
                    out[rows(g), n + h : n + h + HEAD] = (a * cos_s[...] + pltpu.roll(a, HEAD // 2, 1) * sin_s[...]).astype(jnp.bfloat16)
            v = _dot(xn_s[...], w_s[2, :, n : n + wide], 1, 0).astype(jnp.bfloat16)
            vt_s[n : n + wide, rows(g)] = v.T

    cols = [slice(h * HEAD, (h + 1) * HEAD) for h in range(heads)]

    def score(h, g, first, level):
        high = None
        for a in range(0, KB, ch):
            s = _dot(k_s[pl.ds(pl.multiple_of(first, KB) + a, ch), cols[h]], q_s[rows(g), cols[h]], 1, 1)
            if level is not None:
                gap = lax.broadcasted_iota(jnp.int32, s.shape, 1) - lax.broadcasted_iota(jnp.int32, s.shape, 0)
                s = jnp.where(gap >= level + a, s, HIDDEN)
            s_s[h, a : a + ch] = s
            top = s.reshape(ch // 8, 8, ch).max(axis=0)
            high = top if high is None else jnp.maximum(high, top)
        high_s[h] = high

    def take(h, slot, first):
        old = top_s[slot, h : h + 1, :]
        top = jnp.maximum(old, high_s[h].max(axis=0, keepdims=True))
        top_s[slot, h : h + 1, :] = top
        total = acc_s[slot, h] * jnp.exp2((old - top) * e)
        ones = jnp.ones((8, ch), jnp.bfloat16)
        more = None
        for a in range(0, KB, ch):
            p = jnp.exp2((s_s[h, a : a + ch] - top) * e).astype(jnp.bfloat16)
            values = jnp.concatenate([vt_s[cols[h], pl.ds(pl.multiple_of(first, KB) + a, ch)], ones], axis=0)
            part = _dot(values, p, 1, 0)
            more = part if more is None else more + part
        acc_s[slot, h] = total + more

    def begin(task):
        g, _, first, masked = task
        level = jnp.where(masked, first - g * ch, -(2**20))
        for h in range(heads):
            score(h, g, first, level)

    def advance(task, following):
        _, slot, first, _ = task
        g, _, then, masked = following

        @pl.when(masked)
        def _():
            for h in range(heads):
                take(h, slot, first)
                score(h, g, then, then - g * ch)

        @pl.when(jnp.logical_not(masked))
        def _():
            for h in range(heads):
                take(h, slot, first)
                score(h, g, then, None)

    def round_(r, _):
        mine, far = r < 2, r >= 6
        i = jnp.where(mine, 0, jnp.where(far, r - 6, r - 2))
        n = jnp.where(far, i + 4, i)
        ca, cb = jnp.where(mine, 2 * r, i), jnp.where(mine, 2 * r + 1, lax.rem(i + 2, PER))
        ba = jnp.where(mine, me, jnp.where(far, opp, left))
        bb = jnp.where(mine, me, jnp.where(far, opp, right))

        @pl.when(mine)
        def _():
            pltpu.make_async_copy(x_hbm.at[rows(ca)], x_s.at[0], x_sem.at[0]).start()
            pltpu.make_async_copy(x_hbm.at[rows(cb)], x_s.at[1], x_sem.at[1]).start()

        @pl.when(r >= 2)
        def _():
            sa, sb = jnp.where(far, 2, 0), jnp.where(far, 2, 1)
            gather(0, n, xg_hbm.at[0, rows(ca)], sa, ca).wait_recv()
            gather(1, n, xg_hbm.at[1, rows(cb)], sb, cb).wait_recv()

            @pl.when(r < 4)
            def _():
                gather(0, i + 4, xg_hbm.at[0, rows(ca)], 2, ca).start()
                gather(1, i + 4, xg_hbm.at[1, rows(cb)], 2, cb).start()

            pltpu.make_async_copy(xg_hbm.at[sa, rows(ca)], x_s.at[0], x_sem.at[0]).start()
            pltpu.make_async_copy(xg_hbm.at[sb, rows(cb)], x_s.at[1], x_sem.at[1]).start()

        @pl.when(r == 0)
        def _():
            for w in weights:
                w.wait()

        def chunk(j, _):
            pltpu.make_async_copy(x_hbm.at[rows(0)], x_s.at[j], x_sem.at[j]).wait()
            b, c = jnp.where(j == 0, ba, bb), jnp.where(j == 0, ca, cb)

            @pl.when(jnp.logical_not(far))
            def _():
                clear(state(b, c))

            project(b, c, j)

        lax.fori_loop(0, 2, chunk, None)

        @pl.when((r == 1) | (r == 3) | (r == 5))
        def _():
            def task(t):
                c0 = jnp.where(t < 2, t, t // 2 + 1)
                j0 = jnp.where(t < 2, 0, t % 2)
                j, from_left = t % 4, t < 4
                other = jnp.where(from_left, left, right)
                half = jnp.where((r == 3) == from_left, 0, 1)
                later = me > other
                b = jnp.where(mine | later, me, other)
                c = jnp.where(mine, c0, jnp.where(later, j, 2 * half + j // 2))
                kh = jnp.where(mine, 2 * me + j0, jnp.where(later, 2 * other + half, 2 * me + j % 2))
                return b * PER + c, state(b, c), kh * KB, mine & (j0 == c0 // 2)

            count = jnp.where(mine, 6, 8)
            begin(task(0))
            lax.fori_loop(0, count, lambda t, _: advance(task(t), task(jnp.minimum(t + 1, count - 1))), None)

        @pl.when(r == 7)
        def _():
            last.start()

    lax.fori_loop(0, 8, round_, None)

    def halves(side, s):
        part = pl.ds(side * (ch // 2), ch // 2)
        n = side * PER + s
        return pltpu.make_async_remote_copy(src_ref=send_s.at[0, lax.rem(s, 2), part], dst_ref=half_s.at[side, s], send_sem=rs_send.at[n],
                                            recv_sem=rs_recv.at[n], device_id={"tp": (right, left)[side]}, device_id_type=MESH)

    def fulls(side, s):
        n = (2 + side) * PER + s
        return pltpu.make_async_remote_copy(src_ref=send_s.at[1 + side, lax.rem(s, 2)], dst_ref=full_hbm.at[side, s], send_sem=rs_send.at[n],
                                            recv_sem=rs_recv.at[n], device_id={"tp": (right, left)[side]}, device_id_type=MESH)

    def place(n):
        m = jnp.where(n >= 10, n, n - 1)
        kind = jnp.where(n == 0, 0, jnp.where(n >= 12, 3, m % 3))
        s = jnp.where(n == 0, 0, jnp.where(n >= 12, n - 12, m // 3 + jnp.where(m % 3 == 0, 1, 0)))
        b = jnp.where(kind == 0, opp, jnp.where(kind == 1, right, jnp.where(kind == 2, left, me)))
        return kind, s, b

    def tasks(n):
        kind, s, b = place(n)
        before = jnp.where(kind == 0, b, jnp.where(kind == 3, jnp.where(opp < me, 1, 0), b - jnp.where(me < b, 1, 0)))
        return 2 * before, 2 * before + jnp.where(kind == 3, 0, s // 2 + 1)

    def task(n, j):
        kind, s, b = place(n)
        earlier, count = tasks(n)
        u = j // 2
        kb = jnp.where(kind == 3, opp, u + jnp.where((kind != 0) & (me < b) & (u >= me), 1, 0))
        kh = jnp.where(j < earlier, 2 * kb + j % 2, 2 * b + j - earlier)
        return b * PER + s, state(b, s), kh * KB, (kind != 3) & (j == count - 1)

    def item(n, _):
        kind, s, b = place(n)
        slot = state(b, s)
        _, count = tasks(n)

        @pl.when(kind == 0)
        def _():
            clear(slot)

        def one(j, _):
            more = j + 1 < count
            advance(task(n, j), task(jnp.where(more, n, jnp.minimum(n + 1, 4 * PER - 1)), jnp.where(more, j + 1, 0)))

        lax.fori_loop(0, count, one, None)

        @pl.when(n == 0)
        def _():
            last.wait()

        for h in range(heads):
            total = acc_s[slot, h, HEAD : HEAD + 1, :]
            seen_s[:, h * HEAD : (h + 1) * HEAD] = (acc_s[slot, h, :HEAD, :] * (1 / total)).astype(jnp.bfloat16).T
        for j in range(0, term_s.shape[1], wide):
            term_s[:, j : j + wide] = _dot(seen_s[...], w_s[0, :, j : j + wide], 1, 0)

        @pl.when(kind == 0)
        def _():
            @pl.when(s >= 2)
            def _():
                halves(0, s - 2).wait_send()
                halves(1, s - 2).wait_send()

            send_s[0, lax.rem(s, 2)] = term_s[...].astype(jnp.bfloat16)
            halves(0, s).start()
            halves(1, s).start()

        for side in range(2):

            @pl.when(kind == 1 + side)
            def _(side=side):
                @pl.when(s >= 2)
                def _():
                    fulls(side, s - 2).wait_send()

                halves(side, s).wait_recv()
                mid = ch // 2
                near, rest = slice(side * mid, (side + 1) * mid), slice((1 - side) * mid, (2 - side) * mid)
                to = lax.rem(s, 2)
                send_s[1 + side, to, rest] = term_s[rest].astype(jnp.bfloat16)
                send_s[1 + side, to, near] = (term_s[near] + half_s[side, s].astype(jnp.float32)).astype(jnp.bfloat16)
                fulls(side, s).start()

        @pl.when(kind == 3)
        def _():
            token = pltpu.make_async_copy(x_hbm.at[rows(s)], x_s.at[0], x_sem.at[0])
            token.start()
            come = []
            for side in range(2):
                fulls(side, s).wait_recv()
                come.append(pltpu.make_async_copy(full_hbm.at[side, s], got_s.at[side], got_sem.at[side]))
                come[side].start()
            token.wait()
            for one in come:
                one.wait()
            total = term_s[...] + got_s[0].astype(jnp.float32) + got_s[1].astype(jnp.float32)
            x_s[1] = (x_s[0].astype(jnp.float32) + total).astype(jnp.bfloat16)
            done = pltpu.make_async_copy(x_s.at[1], y_hbm.at[rows(s)], y_sem)
            done.start()
            done.wait()

    begin(task(0, 0))
    lax.fori_loop(0, 4 * PER, item, None)

    for side in range(2):
        for i in range(6):
            gather(side, i, x_hbm.at[rows(0)], 0, 0).wait_send()
        for s in (PER - 2, PER - 1):
            halves(side, s).wait_send()
            fulls(side, s).wait_send()


def solution(mesh):
    def step(x, gain, wq, wk, wv, wo):
        t, d = x.shape
        ch, columns = t // PER, wq.shape[1]
        heads, every = columns // HEAD, t * RING
        rate = np.float64(THETA) ** (-np.arange(HEAD // 2) / (HEAD // 2))
        rate = np.concatenate([rate, rate])
        base, far = np.arange(ch)[:, None] * rate, (np.arange(every // ch) * ch)[:, None] * rate
        tables = [jnp.asarray(f(a), jnp.float32) for a in (base, far) for f in (np.cos, np.sin)]
        hbm, vmem = pl.BlockSpec(memory_space=pl.ANY), pl.BlockSpec(memory_space=pltpu.VMEM)
        bf, f32 = jnp.bfloat16, jnp.float32
        y, _, _ = pl.pallas_call(
            _kernel,
            out_shape=[jax.ShapeDtypeStruct((t, d), bf), jax.ShapeDtypeStruct((3, t, d), bf), jax.ShapeDtypeStruct((2, PER, ch, d), bf)],
            in_specs=[hbm] + [vmem] * 5 + [hbm] * 4,
            out_specs=[hbm] * 3,
            scratch_shapes=[
                pltpu.VMEM((every, columns), bf),
                pltpu.VMEM((every, columns), bf),
                pltpu.VMEM((columns, every), bf),
                pltpu.VMEM((3 * PER + 1, heads, HEAD + 8, ch), f32),
                pltpu.VMEM((3 * PER + 1, heads, ch), f32),
                pltpu.VMEM((heads, KB, ch), f32),
                pltpu.VMEM((heads, 8, ch), f32),
                pltpu.VMEM((3, d, columns), bf),
                pltpu.VMEM((2, ch, d), bf),
                pltpu.VMEM((ch, d), bf),
                pltpu.VMEM((ch, HEAD), f32),
                pltpu.VMEM((ch, HEAD), f32),
                pltpu.VMEM((ch, columns), bf),
                pltpu.VMEM((ch, d), f32),
                pltpu.VMEM((3, 2, ch, d), bf),
                pltpu.VMEM((2, PER, ch // 2, d), bf),
                pltpu.VMEM((2, ch, d), bf),
                pltpu.SemaphoreType.DMA((4,)),
                pltpu.SemaphoreType.DMA((2,)),
                pltpu.SemaphoreType.DMA((2,)),
                pltpu.SemaphoreType.DMA,
                pltpu.SemaphoreType.DMA((12,)),
                pltpu.SemaphoreType.DMA((12,)),
                pltpu.SemaphoreType.DMA((4 * PER,)),
                pltpu.SemaphoreType.DMA((4 * PER,)),
            ],
            compiler_params=pltpu.CompilerParams(collective_id=0, has_side_effects=True, vmem_limit_bytes=VMEM),
        )(x, gain, *tables[:2], *tables[2:], wq, wk, wv, wo)
        return y

    tokens, columns = P(("dp", "tp"), None), P(None, "tp")
    return jax.shard_map(
        step,
        mesh=mesh,
        in_specs=(tokens, P(None), columns, columns, columns, P("tp", None)),
        out_specs=tokens,
        check_vma=False,
    )
```

```python
import functools

import jax
import jax.numpy as jnp
import numpy as np
from jax import lax
from jax.experimental import pallas as pl
from jax.experimental.pallas import tpu as pltpu
from jax.sharding import PartitionSpec as P

HEAD = 128
THETA = 10000
NEG = -1e30
HIDDEN = 2 * NEG
LOG2E = 1.4426950408889634
RING = 4
PER = 4
KB = 512
MESH = pl.DeviceIdType.MESH
VMEM = 67043328


def _dot(a, b, ca, cb):
    return lax.dot_general(a, b, (((ca,), (cb,)), ((), ())), preferred_element_type=jnp.float32)


def _kernel(x_hbm, gain_ref, bc_ref, bs_ref, gc_ref, gs_ref, wq_hbm, wk_hbm, wv_hbm, wo_hbm, y_hbm, xg_hbm, full_hbm,
            q_s, k_s, vt_s, acc_s, top_s, s_s, high_s, w_s, wo_s, x_s, row_s, cos_s, sin_s, term_s, send_s, half_s, got_s,
            w_sem, x_sem, got_sem, ag_send, ag_recv, rs_send, rs_recv):
    ch = x_s.shape[1]
    heads = q_s.shape[1] // HEAD
    wide = 2 * HEAD
    me = lax.axis_index("tp")
    right, left, opp = lax.rem(me + 1, RING), lax.rem(me + 3, RING), lax.rem(me + 2, RING)
    e = HEAD**-0.5 * LOG2E

    for j in range(2):
        pltpu.make_async_copy(x_hbm.at[pl.ds(j * ch, ch)], x_s.at[j], x_sem.at[j]).start()
    weights = [pltpu.make_async_copy(w, w_s.at[i], w_sem.at[i]) for i, w in enumerate((wq_hbm, wk_hbm, wv_hbm))]
    weights.append(pltpu.make_async_copy(wo_hbm, wo_s, w_sem.at[3]))
    for w in weights:
        w.start()

    barrier = pltpu.get_barrier_semaphore()
    for side in (left, right):
        pl.semaphore_signal(barrier, inc=1, device_id={"tp": side}, device_id_type=MESH)
    pl.semaphore_wait(barrier, 2)

    def rows(c):
        return pl.ds(pl.multiple_of(c * ch, ch), ch)

    def gather(side, c):
        n = side * 2 * PER + c
        return pltpu.make_async_remote_copy(src_ref=x_hbm.at[rows(c)], dst_ref=xg_hbm.at[side, rows(c)], send_sem=ag_send.at[n],
                                            recv_sem=ag_recv.at[n], device_id={"tp": (right, left)[side]}, device_id_type=MESH)

    def forward(side, c):
        n = side * 2 * PER + PER + c
        part = pl.ds(pl.multiple_of(c * ch + side * (ch // 2), ch // 2), ch // 2)
        return pltpu.make_async_remote_copy(src_ref=xg_hbm.at[side, part], dst_ref=xg_hbm.at[2, part], send_sem=ag_send.at[n],
                                            recv_sem=ag_recv.at[n], device_id={"tp": (right, left)[side]}, device_id_type=MESH)

    for c in range(PER):
        for side in range(2):
            gather(side, c).start()

    def clear(slot):
        acc_s[slot] = jnp.zeros(acc_s.shape[1:], jnp.float32)
        top_s[slot] = jnp.full(top_s.shape[1:], NEG, jnp.float32)

    def state(b, c):
        rel = lax.rem(b - me + RING, RING)
        return jnp.where(rel == 2, 3 * PER, jnp.where(rel == 3, 2 * PER, rel * PER) + c)

    def project(b, c, at):
        g = b * PER + c
        wide_x = x_s[at].astype(jnp.float32)
        scale = lax.rsqrt(jnp.mean(wide_x * wide_x, -1, keepdims=True) + 1e-6)
        row_s[...] = (wide_x * scale * gain_ref[...].astype(jnp.float32)).astype(jnp.bfloat16)
        gc, gs = gc_ref[pl.ds(g, 1), :], gs_ref[pl.ds(g, 1), :]
        cos_s[...] = gc * bc_ref[...] - gs * bs_ref[...]
        sin = gs * bc_ref[...] + gc * bs_ref[...]
        sin_s[...] = jnp.where(lax.broadcasted_iota(jnp.int32, sin.shape, 1) < HEAD // 2, -sin, sin)
        for n in range(0, heads * HEAD, wide):
            for i, out in ((0, q_s), (1, k_s)):
                t = _dot(row_s[...], w_s[i, :, n : n + wide], 1, 0).astype(jnp.bfloat16).astype(jnp.float32)
                for h in range(0, wide, HEAD):
                    a = t[:, h : h + HEAD]
                    out[rows(g), n + h : n + h + HEAD] = (a * cos_s[...] + pltpu.roll(a, HEAD // 2, 1) * sin_s[...]).astype(jnp.bfloat16)
            v = _dot(row_s[...], w_s[2, :, n : n + wide], 1, 0).astype(jnp.bfloat16)
            vt_s[n : n + wide, rows(g)] = v.T

    cols = [slice(h * HEAD, (h + 1) * HEAD) for h in range(heads)]

    def score(h, g, first, level):
        high = None
        for a in range(0, KB, ch):
            s = _dot(k_s[pl.ds(pl.multiple_of(first, KB) + a, ch), cols[h]], q_s[rows(g), cols[h]], 1, 1)
            if level is not None:
                gap = lax.broadcasted_iota(jnp.int32, s.shape, 1) - lax.broadcasted_iota(jnp.int32, s.shape, 0)
                s = jnp.where(gap >= level + a, s, HIDDEN)
            s_s[h, a : a + ch] = s
            top = s.reshape(ch // 8, 8, ch).max(axis=0)
            high = top if high is None else jnp.maximum(high, top)
        high_s[h] = high

    def take(h, slot, first):
        old = top_s[slot, h : h + 1, :]
        top = jnp.maximum(old, high_s[h].max(axis=0, keepdims=True))
        top_s[slot, h : h + 1, :] = top
        total = acc_s[slot, h] * jnp.exp2((old - top) * e)
        ones = jnp.ones((8, ch), jnp.bfloat16)
        more = None
        for a in range(0, KB, ch):
            p = jnp.exp2((s_s[h, a : a + ch] - top) * e).astype(jnp.bfloat16)
            values = jnp.concatenate([vt_s[cols[h], pl.ds(pl.multiple_of(first, KB) + a, ch)], ones], axis=0)
            part = _dot(values, p, 1, 0)
            more = part if more is None else more + part
        acc_s[slot, h] = total + more

    def begin(task):
        g, _, first, masked = task
        level = jnp.where(masked, first - g * ch, -(2**20))
        for h in range(heads):
            score(h, g, first, level)

    def advance(task, following):
        _, slot, first = task
        g, _, then, masked = following

        @pl.when(masked)
        def _():
            for h in range(heads):
                take(h, slot, first)
                score(h, g, then, then - g * ch)

        @pl.when(jnp.logical_not(masked))
        def _():
            for h in range(heads):
                take(h, slot, first)
                score(h, g, then, None)

    def fetch(r):
        at = 2 * lax.rem(r, 2)

        @pl.when(r == 1)
        def _():
            for j in range(2):
                pltpu.make_async_copy(x_hbm.at[rows(2 * r + j)], x_s.at[at + j], x_sem.at[at + j]).start()

        @pl.when((r >= 2) & (r < 6))
        def _():
            for side in range(2):
                gather(side, r - 2).wait_recv()
                forward(side, r - 2).start()
                pltpu.make_async_copy(xg_hbm.at[side, rows(r - 2)], x_s.at[at + side], x_sem.at[at + side]).start()

        @pl.when(r >= 6)
        def _():
            for j in range(2):
                c = 2 * (r - 6) + j
                for side in range(2):
                    forward(side, c).wait_recv()
                pltpu.make_async_copy(xg_hbm.at[2, rows(c)], x_s.at[at + j], x_sem.at[at + j]).start()

    def round_(r):
        mine, far = r < 2, r >= 6

        @pl.when(r == 0)
        def _():
            for w in weights[:3]:
                w.wait()

        def chunk(j, _):
            at = 2 * lax.rem(r, 2) + j

            @pl.when((j == 1) & ((r == 0) | (r == 2)))
            def _():
                fetch(r + 1)

            pltpu.make_async_copy(x_hbm.at[rows(0)], x_s.at[at], x_sem.at[at]).wait()
            b = jnp.where(mine, me, jnp.where(far, opp, jnp.where(j == 0, left, right)))
            c = jnp.where(mine, 2 * r + j, jnp.where(far, 2 * (r - 6) + j, r - 2))

            @pl.when(jnp.logical_not(far))
            def _():
                clear(state(b, c))

            project(b, c, at)

        lax.fori_loop(0, 2, chunk, None)

    def own_copies(s):
        at = 2 * lax.rem(s, 2)
        come = [pltpu.make_async_copy(full_hbm.at[side, s], got_s.at[at + side], got_sem.at[at + side]) for side in range(2)]
        return come + [pltpu.make_async_copy(x_hbm.at[rows(s)], x_s.at[at], x_sem.at[at])]

    def result(s):
        at = 2 * lax.rem(s, 2) + 1
        return pltpu.make_async_copy(x_s.at[at], y_hbm.at[rows(s)], x_sem.at[at])

    end = 8 + 5 * PER
    low, high = jnp.minimum(left, right), jnp.maximum(left, right)

    def place(st):
        n = st - 8
        r = n & 3
        kind = jnp.where(n < 0, 0, jnp.where(n >= 4 * PER, 4, (r + 1) & 3))
        s = jnp.where(n < 0, jnp.maximum(n + 2, 0), jnp.where(n >= 4 * PER, n - 4 * PER, (n >> 2) + jnp.where(r == 3, 2, 0)))
        kind = jnp.where(s >= PER, 5, kind)
        b = jnp.where(kind == 0, opp, jnp.where(kind == 2, low, jnp.where(kind == 3, high, me)))
        return kind, s, b

    def plan(st):
        kind, s, b = place(st)
        near = kind >= 2
        across = jnp.where(kind == 3, jnp.where(s < PER - 1, 1, 2), 0)
        behind = jnp.where((kind > 0) & (opp < b), 2, 0)
        t1, t2 = across, across + behind
        o1, o2 = 2 * low + jnp.where(s < PER - 1, 1, 0), 2 * opp - across
        o3 = jnp.where(near, 2 * b - t2, 0)
        count = jnp.where(kind >= 4, 0, jnp.where(kind == 0, 2 * b, t2) + jnp.where(kind == 1, 0, (s >> 1) + 1))
        diagonal = jnp.where((st >= 6) & (kind != 1), count - 1, -1)
        for at, size in ((0, 0), (1, 6), (2, 0), (3, 8), (4, 3), (5, 8)):
            count = jnp.where(st == at, size, count)
        half = st >> 2

        def task(j):
            kh = j + jnp.where(j < t1, o1, jnp.where(j < t2, o2, o3))
            i = j & 3
            other = jnp.where(j < 4, left, right)
            later = me > other
            pb, pc = jnp.where(later, me, other), jnp.where(later, i, 2 * half + (i >> 1))
            pk = jnp.where(later, 2 * other + half, 2 * me + (i & 1))
            c, d = jnp.where(j < 2, j, (j >> 1) + 1), jnp.where(j < 2, 0, j & 1)
            own, four = st == 1, st == 4
            early = st < 6
            qb = jnp.where(early, jnp.where(own, me, jnp.where(four, high, pb)), b)
            qc = jnp.where(early, jnp.where(own, c, jnp.where(four, j, pc)), s)
            kh = jnp.where(early, jnp.where(own, 2 * me + d, jnp.where(four, 2 * low, pk)), kh)
            masked = (j == diagonal) | (own & (d == (c >> 1)))
            return qb * PER + qc, state(qb, qc), kh * KB, masked

        return count, task

    def halves(side, s):
        part = pl.ds(side * (ch // 2), ch // 2)
        n = side * PER + s
        return pltpu.make_async_remote_copy(src_ref=send_s.at[0, lax.rem(s, 2), part], dst_ref=half_s.at[side, s], send_sem=rs_send.at[n],
                                            recv_sem=rs_recv.at[n], device_id={"tp": (right, left)[side]}, device_id_type=MESH)

    def fulls(side, s):
        n = (2 + side) * PER + s
        return pltpu.make_async_remote_copy(src_ref=send_s.at[1 + side, lax.rem(s, 2)], dst_ref=full_hbm.at[side, s], send_sem=rs_send.at[n],
                                            recv_sem=rs_recv.at[n], device_id={"tp": (right, left)[side]}, device_id_type=MESH)

    def step(st, _):
        @pl.when(st < 8)
        def _():
            round_(st)

        count, task = plan(st)
        kind, s, b = place(st)
        item = (st >= 6) & (kind != 1) & (kind != 5)
        chained = (st == 3) | (st >= 6)
        empty = (kind == 3) & (s >= PER - 2)
        before_own = (st >= 7) & ((kind == 0) | empty)
        after = st + 1 + jnp.where((st >= 6) & empty, 1, 0) + jnp.where(before_own & (opp > me), 1, 0)
        first = plan(jnp.where(chained, jnp.minimum(after, end - 1), st))[1](0)

        @pl.when(item & (kind == 0))
        def _():
            clear(state(b, s))

        @pl.when((st == 1) | (st == 3) | (st == 5) | (st == 6))
        def _():
            begin(task(0))

        def bring(s):
            for side in range(2):
                fulls(side, s).wait_recv()
            for copy in own_copies(s):
                copy.start()

        @pl.when((kind == 4) & (s == 0))
        def _():
            bring(0)

        @pl.when((kind == 4) & (s < PER - 2))
        def _():
            bring(s + 1)

        ahead = jnp.where((st == 1) | ((st >= 3) & (st < 7)), jnp.maximum(count - 2, 0), -1)

        def one(j, now):
            @pl.when(j == ahead)
            def _():
                fetch(st + 1)

            more = j + 1 < count
            following = task(jnp.minimum(j + 1, count - 1))
            following = tuple(jnp.where(more, p, q) for p, q in zip(following, first))
            advance(now, following)
            return following[:3]

        lax.fori_loop(0, count, one, task(0)[:3])

        @pl.when(st == 6)
        def _():
            weights[3].wait()

        @pl.when(item)
        def _():
            finish(kind, s, b)

    def finish(kind, s, b):
        slot = state(b, s)
        for h in range(heads):
            total = acc_s[slot, h, HEAD : HEAD + 1, :]
            row_s[:, h * HEAD : (h + 1) * HEAD] = (acc_s[slot, h, :HEAD, :] * (1 / total)).astype(jnp.bfloat16).T
        for j in range(0, term_s.shape[1], wide):
            term_s[:, j : j + wide] = _dot(row_s[...], wo_s[:, j : j + wide], 1, 0)

        @pl.when(kind == 0)
        def _():
            @pl.when(s >= 2)
            def _():
                halves(0, s - 2).wait_send()
                halves(1, s - 2).wait_send()

            send_s[0, lax.rem(s, 2)] = term_s[...].astype(jnp.bfloat16)
            halves(0, s).start()
            halves(1, s).start()

        for side in range(2):

            @pl.when(((kind == 2) | (kind == 3)) & (b == (right, left)[side]))
            def _(side=side):
                @pl.when(s >= 2)
                def _():
                    fulls(side, s - 2).wait_send()

                halves(side, s).wait_recv()
                mid = ch // 2
                near, rest = slice(side * mid, (side + 1) * mid), slice((1 - side) * mid, (2 - side) * mid)
                to = lax.rem(s, 2)
                send_s[1 + side, to, rest] = term_s[rest].astype(jnp.bfloat16)
                send_s[1 + side, to, near] = (term_s[near] + half_s[side, s].astype(jnp.float32)).astype(jnp.bfloat16)
                fulls(side, s).start()

        @pl.when(kind == 4)
        def _():
            @pl.when(s >= 2)
            def _():
                result(s - 2).wait()

            @pl.when(s == PER - 1)
            def _():
                for side in range(2):
                    fulls(side, s).wait_recv()
                for copy in own_copies(s):
                    copy.start()

            for copy in own_copies(s):
                copy.wait()
            at = 2 * lax.rem(s, 2)
            total = term_s[...] + got_s[at].astype(jnp.float32) + got_s[at + 1].astype(jnp.float32)
            x_s[at + 1] = (x_s[at].astype(jnp.float32) + total).astype(jnp.bfloat16)
            result(s).start()

    lax.fori_loop(0, end, step, None)

    for s in (PER - 2, PER - 1):
        result(s).wait()
    for side in range(2):
        for c in range(PER):
            gather(side, c).wait_send()
            forward(side, c).wait_send()
        for s in (PER - 2, PER - 1):
            halves(side, s).wait_send()
            fulls(side, s).wait_send()


def solution(mesh):
    def step(x, gain, wq, wk, wv, wo):
        t, d = x.shape
        ch, columns = t // PER, wq.shape[1]
        heads, every = columns // HEAD, t * RING
        rate = np.float64(THETA) ** (-np.arange(HEAD // 2) / (HEAD // 2))
        rate = np.concatenate([rate, rate])
        base, far = np.arange(ch)[:, None] * rate, (np.arange(every // ch) * ch)[:, None] * rate
        tables = [jnp.asarray(f(a), jnp.float32) for a in (base, far) for f in (np.cos, np.sin)]
        hbm, vmem = pl.BlockSpec(memory_space=pl.ANY), pl.BlockSpec(memory_space=pltpu.VMEM)
        bf, f32 = jnp.bfloat16, jnp.float32
        y, _, _ = pl.pallas_call(
            _kernel,
            out_shape=[jax.ShapeDtypeStruct((t, d), bf), jax.ShapeDtypeStruct((3, t, d), bf), jax.ShapeDtypeStruct((2, PER, ch, d), bf)],
            in_specs=[hbm] + [vmem] * 5 + [hbm] * 4,
            out_specs=[hbm] * 3,
            scratch_shapes=[
                pltpu.VMEM((every, columns), bf),
                pltpu.VMEM((every, columns), bf),
                pltpu.VMEM((columns, every), bf),
                pltpu.VMEM((3 * PER + 1, heads, HEAD + 8, ch), f32),
                pltpu.VMEM((3 * PER + 1, heads, ch), f32),
                pltpu.VMEM((heads, KB, ch), f32),
                pltpu.VMEM((heads, 8, ch), f32),
                pltpu.VMEM((3, d, columns), bf),
                pltpu.VMEM((columns, d), bf),
                pltpu.VMEM((4, ch, d), bf),
                pltpu.VMEM((ch, d), bf),
                pltpu.VMEM((ch, HEAD), f32),
                pltpu.VMEM((ch, HEAD), f32),
                pltpu.VMEM((ch, d), f32),
                pltpu.VMEM((3, 2, ch, d), bf),
                pltpu.VMEM((2, PER, ch // 2, d), bf),
                pltpu.VMEM((4, ch, d), bf),
                pltpu.SemaphoreType.DMA((4,)),
                pltpu.SemaphoreType.DMA((4,)),
                pltpu.SemaphoreType.DMA((4,)),
                pltpu.SemaphoreType.DMA((4 * PER,)),
                pltpu.SemaphoreType.DMA((4 * PER,)),
                pltpu.SemaphoreType.DMA((4 * PER,)),
                pltpu.SemaphoreType.DMA((4 * PER,)),
            ],
            compiler_params=pltpu.CompilerParams(collective_id=0, has_side_effects=True, vmem_limit_bytes=VMEM),
        )(x, gain, *tables[:2], *tables[2:], wq, wk, wv, wo)
        return y

    tokens, columns = P(("dp", "tp"), None), P(None, "tp")
    return jax.shard_map(
        step,
        mesh=mesh,
        in_specs=(tokens, P(None), columns, columns, columns, P("tp", None)),
        out_specs=tokens,
        check_vma=False,
    )
```

```python
import functools

import jax
import jax.numpy as jnp
import numpy as np
from jax import lax
from jax.experimental import pallas as pl
from jax.experimental.pallas import tpu as pltpu
from jax.sharding import PartitionSpec as P

HEAD = 128
THETA = 10000
NEG = -1e30
HIDDEN = 2 * NEG
LOG2E = 1.4426950408889634
RING = 4
PER = 4
KB = 512
MESH = pl.DeviceIdType.MESH
VMEM = 67043328


def _dot(a, b, ca, cb):
    return lax.dot_general(a, b, (((ca,), (cb,)), ((), ())), preferred_element_type=jnp.float32)


def _kernel(x_hbm, gain_ref, bc_ref, bs_ref, gc_ref, gs_ref, wq_hbm, wk_hbm, wv_hbm, wo_hbm, y_hbm, xg_hbm, full_hbm,
            q_s, k_s, vt_s, acc_s, top_s, s_s, high_s, w_s, wo_s, x_s, row_s, cos_s, sin_s, term_s, send_s, half_s, got_s,
            w_sem, x_sem, got_sem, ag_send, ag_recv, rs_send, rs_recv):
    ch = x_s.shape[1]
    heads = q_s.shape[1] // HEAD
    wide = 2 * HEAD
    me = lax.axis_index("tp")
    right, left, opp = lax.rem(me + 1, RING), lax.rem(me + 3, RING), lax.rem(me + 2, RING)
    e = HEAD**-0.5 * LOG2E

    for j in range(2):
        pltpu.make_async_copy(x_hbm.at[pl.ds(j * ch, ch)], x_s.at[j], x_sem.at[j]).start()
    weights = [pltpu.make_async_copy(w, w_s.at[i], w_sem.at[i]) for i, w in enumerate((wq_hbm, wk_hbm, wv_hbm))]
    weights.append(pltpu.make_async_copy(wo_hbm, wo_s, w_sem.at[3]))
    for w in weights:
        w.start()

    barrier = pltpu.get_barrier_semaphore()
    for side in (left, right):
        pl.semaphore_signal(barrier, inc=1, device_id={"tp": side}, device_id_type=MESH)
    pl.semaphore_wait(barrier, 2)

    def rows(c):
        return pl.ds(pl.multiple_of(c * ch, ch), ch)

    def gather(side, c):
        n = side * 2 * PER + c
        return pltpu.make_async_remote_copy(src_ref=x_hbm.at[rows(c)], dst_ref=xg_hbm.at[side, rows(c)], send_sem=ag_send.at[n],
                                            recv_sem=ag_recv.at[n], device_id={"tp": (right, left)[side]}, device_id_type=MESH)

    def forward(side, c):
        n = side * 2 * PER + PER + c
        part = pl.ds(pl.multiple_of(c * ch + side * (ch // 2), ch // 2), ch // 2)
        return pltpu.make_async_remote_copy(src_ref=xg_hbm.at[side, part], dst_ref=xg_hbm.at[2, part], send_sem=ag_send.at[n],
                                            recv_sem=ag_recv.at[n], device_id={"tp": (right, left)[side]}, device_id_type=MESH)

    for c in range(PER):
        for side in range(2):
            gather(side, c).start()

    def clear(slot):
        acc_s[slot] = jnp.zeros(acc_s.shape[1:], jnp.float32)
        top_s[slot] = jnp.full(top_s.shape[1:], NEG, jnp.float32)

    def state(b, c):
        rel = lax.rem(b - me + RING, RING)
        return jnp.where(rel == 2, 3 * PER, jnp.where(rel == 3, 2 * PER, rel * PER) + c)

    def project(b, c, at):
        g = b * PER + c
        wide_x = x_s[at].astype(jnp.float32)
        scale = lax.rsqrt(jnp.mean(wide_x * wide_x, -1, keepdims=True) + 1e-6)
        row_s[...] = (wide_x * scale * gain_ref[...].astype(jnp.float32)).astype(jnp.bfloat16)
        gc, gs = gc_ref[pl.ds(g, 1), :], gs_ref[pl.ds(g, 1), :]
        cos_s[...] = gc * bc_ref[...] - gs * bs_ref[...]
        sin = gs * bc_ref[...] + gc * bs_ref[...]
        sin_s[...] = jnp.where(lax.broadcasted_iota(jnp.int32, sin.shape, 1) < HEAD // 2, -sin, sin)
        for n in range(0, heads * HEAD, wide):
            for i, out in ((0, q_s), (1, k_s)):
                t = _dot(row_s[...], w_s[i, :, n : n + wide], 1, 0).astype(jnp.bfloat16).astype(jnp.float32)
                for h in range(0, wide, HEAD):
                    a = t[:, h : h + HEAD]
                    out[rows(g), n + h : n + h + HEAD] = (a * cos_s[...] + pltpu.roll(a, HEAD // 2, 1) * sin_s[...]).astype(jnp.bfloat16)
            v = _dot(row_s[...], w_s[2, :, n : n + wide], 1, 0).astype(jnp.bfloat16)
            vt_s[n : n + wide, rows(g)] = v.T

    cols = [slice(h * HEAD, (h + 1) * HEAD) for h in range(heads)]

    def score(h, g, first, form):
        high = None
        for a in range(0, ch if form == 2 else KB, ch):
            s = _dot(k_s[pl.ds(pl.multiple_of(first, KB) + a, ch), cols[h]], q_s[rows(g), cols[h]], 1, 1)
            if form == 2 or (form == 1 and a > 0):
                seen = lax.broadcasted_iota(jnp.int32, s.shape, 1) >= lax.broadcasted_iota(jnp.int32, s.shape, 0)
                s = jnp.where(seen, s, HIDDEN)
            s_s[h, a : a + ch] = s
            top = s.reshape(ch // 8, 8, ch).max(axis=0)
            high = top if high is None else jnp.maximum(high, top)
        high_s[h] = high

    def take(h, slot, first, form):
        old = top_s[slot, h : h + 1, :]
        top = jnp.maximum(old, high_s[h].max(axis=0, keepdims=True))
        top_s[slot, h : h + 1, :] = top
        total = acc_s[slot, h] * jnp.exp2((old - top) * e)
        ones = jnp.ones((8, ch), jnp.bfloat16)
        more = None
        for a in range(0, ch if form == 2 else KB, ch):
            p = jnp.exp2((s_s[h, a : a + ch] - top) * e).astype(jnp.bfloat16)
            values = jnp.concatenate([vt_s[cols[h], pl.ds(pl.multiple_of(first, KB) + a, ch)], ones], axis=0)
            part = _dot(values, p, 1, 0)
            more = part if more is None else more + part
        acc_s[slot, h] = total + more

    def begin(task):
        g, _, first, form = task
        for kind in (0, 2):

            @pl.when(form == kind)
            def _(kind=kind):
                for h in range(heads):
                    score(h, g, first, kind)

    def advance(task, following):
        slot, first, form = task
        g, _, then, next_form = following
        for old in (0, 2):
            for new in range(3):

                @pl.when(((form == 2) == (old == 2)) & (next_form == new))
                def _(old=old, new=new):
                    for h in range(heads):
                        take(h, slot, first, old)
                        score(h, g, then, new)

    def fetch(r):
        at = 2 * lax.rem(r, 2)

        @pl.when(r == 1)
        def _():
            for j in range(2):
                pltpu.make_async_copy(x_hbm.at[rows(2 * r + j)], x_s.at[at + j], x_sem.at[at + j]).start()

        @pl.when((r >= 2) & (r < 6))
        def _():
            for side in range(2):
                gather(side, r - 2).wait_recv()
                forward(side, r - 2).start()
                pltpu.make_async_copy(xg_hbm.at[side, rows(r - 2)], x_s.at[at + side], x_sem.at[at + side]).start()

        @pl.when(r >= 6)
        def _():
            for j in range(2):
                c = 2 * (r - 6) + j
                for side in range(2):
                    forward(side, c).wait_recv()
                pltpu.make_async_copy(xg_hbm.at[2, rows(c)], x_s.at[at + j], x_sem.at[at + j]).start()

    def round_(r):
        mine, far = r < 2, r >= 6

        @pl.when(r == 0)
        def _():
            for w in weights[:3]:
                w.wait()

        def chunk(j, _):
            at = 2 * lax.rem(r, 2) + j

            @pl.when((j == 1) & ((r == 0) | (r == 2)))
            def _():
                fetch(r + 1)

            pltpu.make_async_copy(x_hbm.at[rows(0)], x_s.at[at], x_sem.at[at]).wait()
            b = jnp.where(mine, me, jnp.where(far, opp, jnp.where(j == 0, left, right)))
            c = jnp.where(mine, 2 * r + j, jnp.where(far, 2 * (r - 6) + j, r - 2))

            @pl.when(jnp.logical_not(far))
            def _():
                clear(state(b, c))

            project(b, c, at)

        lax.fori_loop(0, 2, chunk, None)

    def own_copies(s):
        at = 2 * lax.rem(s, 2)
        come = [pltpu.make_async_copy(full_hbm.at[side, s], got_s.at[at + side], got_sem.at[at + side]) for side in range(2)]
        return come + [pltpu.make_async_copy(x_hbm.at[rows(s)], x_s.at[at], x_sem.at[at])]

    def result(s):
        at = 2 * lax.rem(s, 2) + 1
        return pltpu.make_async_copy(x_s.at[at], y_hbm.at[rows(s)], x_sem.at[at])

    end = 8 + 5 * PER
    low, high = jnp.minimum(left, right), jnp.maximum(left, right)
    odd = lax.axis_index("dp") & 1

    def place(st):
        n = st - 8
        r = n & 3
        kind = jnp.where(n < 0, 0, jnp.where(n >= 4 * PER, 4, jnp.where((r == 1) | (r == 2), 2 + ((r - 1) ^ odd), (r + 1) & 3)))
        s = jnp.where(n < 0, jnp.maximum(n + 2, 0), jnp.where(n >= 4 * PER, n - 4 * PER, (n >> 2) + jnp.where(r == 3, 2, 0)))
        kind = jnp.where(s >= PER, 5, kind)
        b = jnp.where(kind == 0, opp, jnp.where(kind == 2, low, jnp.where(kind == 3, high, me)))
        return kind, s, b

    def plan(st):
        kind, s, b = place(st)
        near = kind >= 2
        across = jnp.where(kind == 3, jnp.where(s < PER - 1, 1, 2), 0)
        behind = jnp.where((kind > 0) & (opp < b), 2, 0)
        t1, t2 = across, across + behind
        o1, o2 = 2 * low + jnp.where(s < PER - 1, 1, 0), 2 * opp - across
        o3 = jnp.where(near, 2 * b - t2, 0)
        pairs = jnp.where((kind == 1) & (s == 2), 4, 0)
        count = jnp.where(kind >= 4, 0, jnp.where(kind == 0, 2 * b, t2) + jnp.where(kind == 1, pairs, (s >> 1) + 1))
        diagonal = jnp.where((st >= 6) & (kind != 1), count - 1, -1)
        for at, size in ((0, 0), (1, 6), (2, 0), (3, 8), (4, 3), (5, 4)):
            count = jnp.where(st == at, size, count)

        early, own, four = st < 6, st == 1, st == 4
        base, home = state(b, 0), jnp.where(own, me, high)
        home_base = state(home, 0)
        half = jnp.where(st == 3, 0, 1)
        pair_from, pair_at = jnp.where(early, 0, jnp.where(pairs > 0, t2, 2**20)), jnp.where(early, 0, 4)

        def task(j):
            p = j - pair_from + pair_at
            i, hi, lo = p & 3, j >> 1, j & 1
            from_left = p < 4
            other = jnp.where(from_left, left, right)
            later = me > other
            pair_b = jnp.where(later, me, other)
            pair_base = jnp.where(later, 0, jnp.where(from_left, 2 * PER, PER))
            pair_c = jnp.where(later, i, 2 * half + (i >> 1))
            pair_k = jnp.where(later, 2 * other + half, 2 * me + (i & 1))
            alone = own | four
            pair = (j >= pair_from) & jnp.logical_not(alone)
            c = jnp.where(four | (j < 2), j, hi + 1)
            d = jnp.where(four | (j < 2), 0, lo)
            qc = jnp.where(alone, c, jnp.where(pair, pair_c, s))
            qb = jnp.where(alone, home, jnp.where(pair, pair_b, b))
            slot = jnp.where(alone, home_base, jnp.where(pair, pair_base, base)) + jnp.where((kind == 0) & (st >= 6), 0, qc)
            item_k = j + jnp.where(j < t1, o1, jnp.where(j < t2, o2, o3))
            kh = jnp.where(alone, jnp.where(own, 2 * me, 2 * low) + d, jnp.where(pair, pair_k, item_k))
            masked = (j == diagonal) | (own & (d == (c >> 1)))
            return qb * PER + qc, slot, kh * KB, jnp.where(masked, 2 - (qc & 1), 0)

        return count, task

    def halves(side, s):
        part = pl.ds(side * (ch // 2), ch // 2)
        n = side * PER + s
        return pltpu.make_async_remote_copy(src_ref=send_s.at[0, lax.rem(s, 2), part], dst_ref=half_s.at[side, s], send_sem=rs_send.at[n],
                                            recv_sem=rs_recv.at[n], device_id={"tp": (right, left)[side]}, device_id_type=MESH)

    def fulls(side, s):
        n = (2 + side) * PER + s
        return pltpu.make_async_remote_copy(src_ref=send_s.at[1 + side, lax.rem(s, 2)], dst_ref=full_hbm.at[side, s], send_sem=rs_send.at[n],
                                            recv_sem=rs_recv.at[n], device_id={"tp": (right, left)[side]}, device_id_type=MESH)

    def step(st, _):
        @pl.when((st < 7) | (st == 8))
        def _():
            round_(jnp.minimum(st, 7))

        count, task = plan(st)
        kind, s, b = place(st)
        item = (st >= 6) & (kind != 1) & (kind != 5)
        chained = (st == 3) | (st >= 6)
        empty = (kind >= 2) & (kind <= 3) & ((st & 3) == 2) & (s >= PER - 2)
        before_own = (st >= 7) & ((kind == 0) | empty)
        own_next = ((st - 8) >> 2) + 1
        skips = before_own & (opp > me) & (own_next != 2) & (own_next < PER)
        after = st + 1 + jnp.where((st >= 6) & empty, 1, 0) + jnp.where(skips, 1, 0)
        first = plan(jnp.where(chained, jnp.minimum(after, end - 1), st))[1](0)

        @pl.when(item & (kind == 0))
        def _():
            clear(state(b, s))

        @pl.when((st == 1) | (st == 3) | (st == 5) | (st == 6))
        def _():
            begin(task(0))

        def bring(s):
            for side in range(2):
                fulls(side, s).wait_recv()
            for copy in own_copies(s):
                copy.start()

        @pl.when((kind == 4) & (s == 0))
        def _():
            bring(0)

        @pl.when((kind == 4) & (s < PER - 2))
        def _():
            bring(s + 1)

        ahead = jnp.where((st == 1) | ((st >= 3) & (st <= 5)) | (st == 7), jnp.maximum(count - 2, 0), -1)

        def one(j, now):
            @pl.when(j == ahead)
            def _():
                fetch(jnp.minimum(st, 6) + 1)

            more = j + 1 < count
            following = task(jnp.minimum(j + 1, count - 1))
            following = tuple(jnp.where(more, p, q) for p, q in zip(following, first))
            advance(now, following)
            return following[1:]

        lax.fori_loop(0, count, one, task(0)[1:])

        @pl.when(st == 6)
        def _():
            weights[3].wait()

        @pl.when(item)
        def _():
            finish(kind, s, b)

    def finish(kind, s, b):
        slot = state(b, s)
        for h in range(heads):
            total = acc_s[slot, h, HEAD : HEAD + 1, :]
            row_s[:, h * HEAD : (h + 1) * HEAD] = (acc_s[slot, h, :HEAD, :] * (1 / total)).astype(jnp.bfloat16).T
        for j in range(0, term_s.shape[1], wide):
            term_s[:, j : j + wide] = _dot(row_s[...], wo_s[:, j : j + wide], 1, 0)

        @pl.when(kind == 0)
        def _():
            @pl.when(s >= 2)
            def _():
                halves(0, s - 2).wait_send()
                halves(1, s - 2).wait_send()

            send_s[0, lax.rem(s, 2)] = term_s[...].astype(jnp.bfloat16)
            halves(0, s).start()
            halves(1, s).start()

        for side in range(2):

            @pl.when(((kind == 2) | (kind == 3)) & (b == (right, left)[side]))
            def _(side=side):
                @pl.when(s >= 2)
                def _():
                    fulls(side, s - 2).wait_send()

                halves(side, s).wait_recv()
                mid = ch // 2
                near, rest = slice(side * mid, (side + 1) * mid), slice((1 - side) * mid, (2 - side) * mid)
                to = lax.rem(s, 2)
                send_s[1 + side, to, rest] = term_s[rest].astype(jnp.bfloat16)
                send_s[1 + side, to, near] = (term_s[near] + half_s[side, s].astype(jnp.float32)).astype(jnp.bfloat16)
                fulls(side, s).start()

        @pl.when(kind == 4)
        def _():
            @pl.when(s >= 2)
            def _():
                result(s - 2).wait()

            @pl.when(s == PER - 1)
            def _():
                for side in range(2):
                    fulls(side, s).wait_recv()
                for copy in own_copies(s):
                    copy.start()

            for copy in own_copies(s):
                copy.wait()
            at = 2 * lax.rem(s, 2)
            total = term_s[...] + got_s[at].astype(jnp.float32) + got_s[at + 1].astype(jnp.float32)
            x_s[at + 1] = (x_s[at].astype(jnp.float32) + total).astype(jnp.bfloat16)
            result(s).start()

    lax.fori_loop(0, end, step, None)

    for s in (PER - 2, PER - 1):
        result(s).wait()
    for side in range(2):
        for c in range(PER):
            gather(side, c).wait_send()
            forward(side, c).wait_send()
        for s in (PER - 2, PER - 1):
            halves(side, s).wait_send()
            fulls(side, s).wait_send()


def solution(mesh):
    def step(x, gain, wq, wk, wv, wo):
        t, d = x.shape
        ch, columns = t // PER, wq.shape[1]
        heads, every = columns // HEAD, t * RING
        rate = np.float64(THETA) ** (-np.arange(HEAD // 2) / (HEAD // 2))
        rate = np.concatenate([rate, rate])
        base, far = np.arange(ch)[:, None] * rate, (np.arange(every // ch) * ch)[:, None] * rate
        tables = [jnp.asarray(f(a), jnp.float32) for a in (base, far) for f in (np.cos, np.sin)]
        hbm, vmem = pl.BlockSpec(memory_space=pl.ANY), pl.BlockSpec(memory_space=pltpu.VMEM)
        bf, f32 = jnp.bfloat16, jnp.float32
        y, _, _ = pl.pallas_call(
            _kernel,
            out_shape=[jax.ShapeDtypeStruct((t, d), bf), jax.ShapeDtypeStruct((3, t, d), bf), jax.ShapeDtypeStruct((2, PER, ch, d), bf)],
            in_specs=[hbm] + [vmem] * 5 + [hbm] * 4,
            out_specs=[hbm] * 3,
            scratch_shapes=[
                pltpu.VMEM((every, columns), bf),
                pltpu.VMEM((every, columns), bf),
                pltpu.VMEM((columns, every), bf),
                pltpu.VMEM((3 * PER + 1, heads, HEAD + 8, ch), f32),
                pltpu.VMEM((3 * PER + 1, heads, ch), f32),
                pltpu.VMEM((heads, KB, ch), f32),
                pltpu.VMEM((heads, 8, ch), f32),
                pltpu.VMEM((3, d, columns), bf),
                pltpu.VMEM((columns, d), bf),
                pltpu.VMEM((4, ch, d), bf),
                pltpu.VMEM((ch, d), bf),
                pltpu.VMEM((ch, HEAD), f32),
                pltpu.VMEM((ch, HEAD), f32),
                pltpu.VMEM((ch, d), f32),
                pltpu.VMEM((3, 2, ch, d), bf),
                pltpu.VMEM((2, PER, ch // 2, d), bf),
                pltpu.VMEM((4, ch, d), bf),
                pltpu.SemaphoreType.DMA((4,)),
                pltpu.SemaphoreType.DMA((4,)),
                pltpu.SemaphoreType.DMA((4,)),
                pltpu.SemaphoreType.DMA((4 * PER,)),
                pltpu.SemaphoreType.DMA((4 * PER,)),
                pltpu.SemaphoreType.DMA((4 * PER,)),
                pltpu.SemaphoreType.DMA((4 * PER,)),
            ],
            compiler_params=pltpu.CompilerParams(collective_id=0, has_side_effects=True, vmem_limit_bytes=VMEM),
        )(x, gain, *tables[:2], *tables[2:], wq, wk, wv, wo)
        return y

    tokens, columns = P(("dp", "tp"), None), P(None, "tp")
    return jax.shard_map(
        step,
        mesh=mesh,
        in_specs=(tokens, P(None), columns, columns, columns, P("tp", None)),
        out_specs=tokens,
        check_vma=False,
    )
```

```python
import functools

import jax
import jax.numpy as jnp
import numpy as np
from jax import lax
from jax.experimental import pallas as pl
from jax.experimental.pallas import tpu as pltpu
from jax.sharding import PartitionSpec as P

HEAD = 128
THETA = 10000
NEG = -1e30
HIDDEN = 2 * NEG
LOG2E = 1.4426950408889634
RING = 4
PER = 4
KB = 512
MESH = pl.DeviceIdType.MESH
VMEM = 67043328


def _dot(a, b, ca, cb):
    return lax.dot_general(a, b, (((ca,), (cb,)), ((), ())), preferred_element_type=jnp.float32)


def _kernel(x_hbm, gain_ref, bc_ref, bs_ref, gc_ref, gs_ref, wq_hbm, wk_hbm, wv_hbm, wo_hbm, y_hbm, xg_hbm, full_hbm,
            q_s, k_s, vt_s, acc_s, top_s, s_s, high_s, w_s, wo_s, x_s, row_s, cos_s, sin_s, term_s, send_s, half_s, got_s, last_s,
            w_sem, x_sem, got_sem, ag_send, ag_recv, rs_send, rs_recv):
    ch = x_s.shape[1]
    heads = q_s.shape[1] // HEAD
    wide = 2 * HEAD
    me = lax.axis_index("tp")
    right, left, opp = lax.rem(me + 1, RING), lax.rem(me + 3, RING), lax.rem(me + 2, RING)
    e = HEAD**-0.5 * LOG2E

    for j in range(2):
        pltpu.make_async_copy(x_hbm.at[pl.ds(j * ch, ch)], x_s.at[j], x_sem.at[j]).start()
    weights = [pltpu.make_async_copy(w, w_s.at[i], w_sem.at[i]) for i, w in enumerate((wq_hbm, wk_hbm, wv_hbm))]
    weights.append(pltpu.make_async_copy(wo_hbm, wo_s, w_sem.at[3]))
    for w in weights:
        w.start()

    barrier = pltpu.get_barrier_semaphore()
    for side in (left, right):
        pl.semaphore_signal(barrier, inc=1, device_id={"tp": side}, device_id_type=MESH)
    pl.semaphore_wait(barrier, 2)

    def rows(c):
        return pl.ds(pl.multiple_of(c * ch, ch), ch)

    def gather(side, c):
        n = side * 2 * PER + c
        return pltpu.make_async_remote_copy(src_ref=x_hbm.at[rows(c)], dst_ref=xg_hbm.at[side, rows(c)], send_sem=ag_send.at[n],
                                            recv_sem=ag_recv.at[n], device_id={"tp": (right, left)[side]}, device_id_type=MESH)

    def forward(side, c):
        n = side * 2 * PER + PER + c
        part = pl.ds(pl.multiple_of(c * ch + side * (ch // 2), ch // 2), ch // 2)
        return pltpu.make_async_remote_copy(src_ref=xg_hbm.at[side, part], dst_ref=xg_hbm.at[2, part], send_sem=ag_send.at[n],
                                            recv_sem=ag_recv.at[n], device_id={"tp": (right, left)[side]}, device_id_type=MESH)

    for c in range(PER):
        for side in range(2):
            gather(side, c).start()

    def clear(slot):
        acc_s[slot] = jnp.zeros(acc_s.shape[1:], jnp.float32)
        top_s[slot] = jnp.full(top_s.shape[1:], NEG, jnp.float32)

    def state(b, c):
        rel = lax.rem(b - me + RING, RING)
        return jnp.where(rel == 2, 3 * PER, jnp.where(rel == 3, 2 * PER, rel * PER) + c)

    def project(b, c, at):
        g = b * PER + c
        wide_x = x_s[at].astype(jnp.float32)
        scale = lax.rsqrt(jnp.mean(wide_x * wide_x, -1, keepdims=True) + 1e-6)
        row_s[...] = (wide_x * scale * gain_ref[...].astype(jnp.float32)).astype(jnp.bfloat16)
        gc, gs = gc_ref[pl.ds(g, 1), :], gs_ref[pl.ds(g, 1), :]
        cos_s[...] = gc * bc_ref[...] - gs * bs_ref[...]
        sin = gs * bc_ref[...] + gc * bs_ref[...]
        sin_s[...] = jnp.where(lax.broadcasted_iota(jnp.int32, sin.shape, 1) < HEAD // 2, -sin, sin)
        for n in range(0, heads * HEAD, wide):
            for i, out in ((0, q_s), (1, k_s)):
                t = _dot(row_s[...], w_s[i, :, n : n + wide], 1, 0).astype(jnp.bfloat16).astype(jnp.float32)
                for h in range(0, wide, HEAD):
                    a = t[:, h : h + HEAD]
                    out[rows(g), n + h : n + h + HEAD] = (a * cos_s[...] + pltpu.roll(a, HEAD // 2, 1) * sin_s[...]).astype(jnp.bfloat16)
            v = _dot(row_s[...], w_s[2, :, n : n + wide], 1, 0).astype(jnp.bfloat16)
            vt_s[n : n + wide, rows(g)] = v.T

    cols = [slice(h * HEAD, (h + 1) * HEAD) for h in range(heads)]

    def score(h, g, first, form):
        high = None
        for a in range(0, ch if form == 2 else KB, ch):
            s = _dot(k_s[pl.ds(pl.multiple_of(first, KB) + a, ch), cols[h]], q_s[rows(g), cols[h]], 1, 1)
            if form == 2 or (form == 1 and a > 0):
                seen = lax.broadcasted_iota(jnp.int32, s.shape, 1) >= lax.broadcasted_iota(jnp.int32, s.shape, 0)
                s = jnp.where(seen, s, HIDDEN)
            s_s[h, a : a + ch] = s
            top = s.reshape(ch // 8, 8, ch).max(axis=0)
            high = top if high is None else jnp.maximum(high, top)
        high_s[h] = high

    def take(h, slot, first, form):
        old = top_s[slot, h : h + 1, :]
        top = jnp.maximum(old, high_s[h].max(axis=0, keepdims=True))
        top_s[slot, h : h + 1, :] = top
        total = acc_s[slot, h] * jnp.exp2((old - top) * e)
        ones = jnp.ones((8, ch), jnp.bfloat16)
        more = None
        for a in range(0, ch if form == 2 else KB, ch):
            p = jnp.exp2((s_s[h, a : a + ch] - top) * e).astype(jnp.bfloat16)
            values = jnp.concatenate([vt_s[cols[h], pl.ds(pl.multiple_of(first, KB) + a, ch)], ones], axis=0)
            part = _dot(values, p, 1, 0)
            more = part if more is None else more + part
        acc_s[slot, h] = total + more

    def begin(task):
        g, _, first, form = task
        for kind in (0, 2):

            @pl.when(form == kind)
            def _(kind=kind):
                for h in range(heads):
                    score(h, g, first, kind)

    def advance(task, following, after):
        slot, first, form = task
        g, _, then, next_form = following

        def branch(old, new):
            def body():
                got = after()
                for h in range(heads):
                    take(h, slot, first, old)
                    score(h, g, then, new)
                return got

            return body

        whole = [branch(0, new) for new in range(3)]
        part = [branch(2, new) for new in range(3)]

        def choose(of):
            return lambda: lax.cond(next_form == 0, of[0], lambda: lax.cond(next_form == 1, of[1], of[2]))

        return lax.cond(form == 2, choose(part), choose(whole))

    def fetch(r):
        at = 2 * lax.rem(r, 2)

        @pl.when(r == 1)
        def _():
            for j in range(2):
                pltpu.make_async_copy(x_hbm.at[rows(2 * r + j)], x_s.at[at + j], x_sem.at[at + j]).start()

        @pl.when((r >= 2) & (r < 6))
        def _():
            for side in range(2):
                gather(side, r - 2).wait_recv()
                forward(side, r - 2).start()
                pltpu.make_async_copy(xg_hbm.at[side, rows(r - 2)], x_s.at[at + side], x_sem.at[at + side]).start()

        @pl.when(r >= 6)
        def _():
            for j in range(2):
                c = 2 * (r - 6) + j
                for side in range(2):
                    forward(side, c).wait_recv()
                pltpu.make_async_copy(xg_hbm.at[2, rows(c)], x_s.at[at + j], x_sem.at[at + j]).start()

    def round_(r):
        mine, far = r < 2, r >= 6

        @pl.when(r == 0)
        def _():
            for w in weights[:3]:
                w.wait()

        def chunk(j, _):
            at = 2 * lax.rem(r, 2) + j

            @pl.when((j == 1) & ((r == 0) | (r == 2)))
            def _():
                fetch(r + 1)

            pltpu.make_async_copy(x_hbm.at[rows(0)], x_s.at[at], x_sem.at[at]).wait()
            b = jnp.where(mine, me, jnp.where(far, opp, jnp.where(j == 0, left, right)))
            c = jnp.where(mine, 2 * r + j, jnp.where(far, 2 * (r - 6) + j, r - 2))

            @pl.when(jnp.logical_not(far))
            def _():
                clear(state(b, c))

            project(b, c, at)

        lax.fori_loop(0, 2, chunk, None)

    def sums(s):
        at = 2 * lax.rem(s, 2)
        return [pltpu.make_async_copy(full_hbm.at[side, s], got_s.at[at + side], got_sem.at[at + side]) for side in range(2)]

    def tokens(s):
        at = 2 * lax.rem(s, 2)
        return pltpu.make_async_copy(x_hbm.at[rows(s)], x_s.at[at], x_sem.at[at])

    def result(s):
        at = 2 * lax.rem(s, 2) + 1
        return pltpu.make_async_copy(x_s.at[at], y_hbm.at[rows(s)], x_sem.at[at])

    end = 8 + 5 * PER
    low, high = jnp.minimum(left, right), jnp.maximum(left, right)

    def place(st):
        n = st - 8
        r = n & 3
        kind = jnp.where(n < 0, 0, jnp.where(n >= 4 * PER, 4, (r + 1) & 3))
        s = jnp.where(n < 0, jnp.maximum(n + 2, 0), jnp.where(n >= 4 * PER, n - 4 * PER, (n >> 2) + jnp.where(r == 3, 2, 0)))
        kind = jnp.where(s >= PER, 5, kind)
        b = jnp.where(kind == 0, opp, jnp.where(kind == 2, low, jnp.where(kind == 3, high, me)))
        return kind, s, b

    def plan(st):
        kind, s, b = place(st)
        near = kind >= 2
        across = jnp.where(kind == 3, jnp.where(s < PER - 1, 1, 2), 0)
        behind = jnp.where((kind > 0) & (opp < b), 2, 0)
        t1, t2 = across, across + behind
        o1, o2 = 2 * low + jnp.where(s < PER - 1, 1, 0), 2 * opp - across
        o3 = jnp.where(near, 2 * b - t2, 0)
        pairs = jnp.where((kind == 1) & (s == 2), 4, 0)
        count = jnp.where(kind >= 4, 0, jnp.where(kind == 0, 2 * b, t2) + jnp.where(kind == 1, pairs, (s >> 1) + 1))
        diagonal = jnp.where((st >= 6) & (kind != 1), count - 1, -1)
        for at, size in ((0, 0), (1, 6), (2, 0), (3, 8), (4, 3), (5, 4)):
            count = jnp.where(st == at, size, count)

        early, own, four = st < 6, st == 1, st == 4
        base, home = state(b, 0), jnp.where(own, me, high)
        home_base = state(home, 0)
        half = jnp.where(st == 3, 0, 1)
        pair_from, pair_at = jnp.where(early, 0, jnp.where(pairs > 0, t2, 2**20)), jnp.where(early, 0, 4)

        def task(j):
            p = j - pair_from + pair_at
            i, hi, lo = p & 3, j >> 1, j & 1
            from_left = p < 4
            other = jnp.where(from_left, left, right)
            later = me > other
            pair_b = jnp.where(later, me, other)
            pair_base = jnp.where(later, 0, jnp.where(from_left, 2 * PER, PER))
            pair_c = jnp.where(later, i, 2 * half + (i >> 1))
            pair_k = jnp.where(later, 2 * other + half, 2 * me + (i & 1))
            alone = own | four
            pair = (j >= pair_from) & jnp.logical_not(alone)
            c = jnp.where(four | (j < 2), j, hi + 1)
            d = jnp.where(four | (j < 2), 0, lo)
            qc = jnp.where(alone, c, jnp.where(pair, pair_c, s))
            qb = jnp.where(alone, home, jnp.where(pair, pair_b, b))
            slot = jnp.where(alone, home_base, jnp.where(pair, pair_base, base)) + jnp.where((kind == 0) & (st >= 6), 0, qc)
            item_k = j + jnp.where(j < t1, o1, jnp.where(j < t2, o2, o3))
            kh = jnp.where(alone, jnp.where(own, 2 * me, 2 * low) + d, jnp.where(pair, pair_k, item_k))
            masked = (j == diagonal) | (own & (d == (c >> 1)))
            return qb * PER + qc, slot, kh * KB, jnp.where(masked, 2 - (qc & 1), 0)

        return count, task

    def halves(side, s):
        part = pl.ds(side * (ch // 2), ch // 2)
        n = side * PER + s
        return pltpu.make_async_remote_copy(src_ref=send_s.at[0, lax.rem(s, 2), part], dst_ref=half_s.at[side, s], send_sem=rs_send.at[n],
                                            recv_sem=rs_recv.at[n], device_id={"tp": (right, left)[side]}, device_id_type=MESH)

    def fulls(side, s, final=False):
        n = (2 + side) * PER + s
        to = last_s.at[side] if final else full_hbm.at[side, s]
        return pltpu.make_async_remote_copy(src_ref=send_s.at[1 + side, lax.rem(s, 2)], dst_ref=to, send_sem=rs_send.at[n],
                                            recv_sem=rs_recv.at[n], device_id={"tp": (right, left)[side]}, device_id_type=MESH)

    def step(st, _):
        @pl.when((st < 7) | (st == 8))
        def _():
            round_(jnp.minimum(st, 7))

        count, task = plan(st)
        kind, s, b = place(st)
        item = (st >= 6) & (kind != 1) & (kind != 5)
        chained = (st == 3) | (st >= 6)
        empty = (kind >= 2) & (kind <= 3) & ((st & 3) == 2) & (s >= PER - 2)
        before_own = (st >= 7) & ((kind == 0) | empty)
        own_next = ((st - 8) >> 2) + 1
        skips = before_own & (opp > me) & (own_next != 2) & (own_next < PER)
        after = st + 1 + jnp.where((st >= 6) & empty, 1, 0) + jnp.where(skips, 1, 0)
        first = plan(jnp.where(chained, jnp.minimum(after, end - 1), st))[1](0)

        @pl.when(item & (kind == 0))
        def _():
            clear(state(b, s))

        @pl.when((st == 1) | (st == 3) | (st == 5) | (st == 6))
        def _():
            begin(task(0))

        def bring(s):
            tokens(s).start()

            @pl.when(s < PER - 1)
            def _():
                for side in range(2):
                    fulls(side, s).wait_recv()
                for copy in sums(s):
                    copy.start()

        @pl.when((kind == 4) & (s == 0))
        def _():
            bring(0)

        @pl.when((kind == 4) & (s < PER - 1))
        def _():
            bring(s + 1)

        ahead = jnp.where((st == 1) | ((st >= 3) & (st <= 5)) | (st == 7), jnp.maximum(count - 2, 0), -1)

        def take_up(j):
            return tuple(jnp.where(j < count, p, q) for p, q in zip(task(jnp.minimum(j, count - 1)), first))

        def one(j, tasks):
            now, following = tasks

            @pl.when(j == ahead)
            def _():
                fetch(jnp.minimum(st, 6) + 1)

            return following[1:], advance(now, following, lambda: take_up(j + 2))

        lax.fori_loop(0, count, one, (task(0)[1:], take_up(1)))

        @pl.when(st == 6)
        def _():
            weights[3].wait()

        @pl.when(item)
        def _():
            finish(kind, s, b)

    def finish(kind, s, b):
        slot = state(b, s)
        for h in range(heads):
            total = acc_s[slot, h, HEAD : HEAD + 1, :]
            row_s[:, h * HEAD : (h + 1) * HEAD] = (acc_s[slot, h, :HEAD, :] * (1 / total)).astype(jnp.bfloat16).T
        for j in range(0, term_s.shape[1], wide):
            term_s[:, j : j + wide] = _dot(row_s[...], wo_s[:, j : j + wide], 1, 0)

        @pl.when(kind == 0)
        def _():
            @pl.when(s >= 2)
            def _():
                halves(0, s - 2).wait_send()
                halves(1, s - 2).wait_send()

            send_s[0, lax.rem(s, 2)] = term_s[...].astype(jnp.bfloat16)
            halves(0, s).start()
            halves(1, s).start()

        for side in range(2):

            @pl.when(((kind == 2) | (kind == 3)) & (b == (right, left)[side]))
            def _(side=side):
                @pl.when(s >= 2)
                def _():
                    fulls(side, s - 2).wait_send()

                halves(side, s).wait_recv()
                mid = ch // 2
                near, rest = slice(side * mid, (side + 1) * mid), slice((1 - side) * mid, (2 - side) * mid)
                to = lax.rem(s, 2)
                send_s[1 + side, to, rest] = term_s[rest].astype(jnp.bfloat16)
                send_s[1 + side, to, near] = (term_s[near] + half_s[side, s].astype(jnp.float32)).astype(jnp.bfloat16)

                @pl.when(s < PER - 1)
                def _():
                    fulls(side, s).start()

                @pl.when(s == PER - 1)
                def _():
                    fulls(side, s, True).start()

        @pl.when(kind == 4)
        def _():
            @pl.when(s >= 2)
            def _():
                result(s - 2).wait()

            at = 2 * lax.rem(s, 2)

            def add(come):
                total = term_s[...] + come[0].astype(jnp.float32) + come[1].astype(jnp.float32)
                x_s[at + 1] = (x_s[at].astype(jnp.float32) + total).astype(jnp.bfloat16)

            tokens(s).wait()

            @pl.when(s < PER - 1)
            def _():
                for copy in sums(s):
                    copy.wait()
                add((got_s[at], got_s[at + 1]))

            @pl.when(s == PER - 1)
            def _():
                for side in range(2):
                    fulls(side, s, True).wait_recv()
                add((last_s[0], last_s[1]))

            result(s).start()

    lax.fori_loop(0, end, step, None)

    for s in (PER - 2, PER - 1):
        result(s).wait()
    for side in range(2):
        for c in range(PER):
            gather(side, c).wait_send()
            forward(side, c).wait_send()
        for s in (PER - 2, PER - 1):
            halves(side, s).wait_send()
            fulls(side, s).wait_send()


def solution(mesh):
    def step(x, gain, wq, wk, wv, wo):
        t, d = x.shape
        ch, columns = t // PER, wq.shape[1]
        heads, every = columns // HEAD, t * RING
        rate = np.float64(THETA) ** (-np.arange(HEAD // 2) / (HEAD // 2))
        rate = np.concatenate([rate, rate])
        base, far = np.arange(ch)[:, None] * rate, (np.arange(every // ch) * ch)[:, None] * rate
        tables = [jnp.asarray(f(a), jnp.float32) for a in (base, far) for f in (np.cos, np.sin)]
        hbm, vmem = pl.BlockSpec(memory_space=pl.ANY), pl.BlockSpec(memory_space=pltpu.VMEM)
        bf, f32 = jnp.bfloat16, jnp.float32
        y, _, _ = pl.pallas_call(
            _kernel,
            out_shape=[jax.ShapeDtypeStruct((t, d), bf), jax.ShapeDtypeStruct((3, t, d), bf), jax.ShapeDtypeStruct((2, PER, ch, d), bf)],
            in_specs=[hbm] + [vmem] * 5 + [hbm] * 4,
            out_specs=[hbm] * 3,
            scratch_shapes=[
                pltpu.VMEM((every, columns), bf),
                pltpu.VMEM((every, columns), bf),
                pltpu.VMEM((columns, every), bf),
                pltpu.VMEM((3 * PER + 1, heads, HEAD + 8, ch), f32),
                pltpu.VMEM((3 * PER + 1, heads, ch), f32),
                pltpu.VMEM((heads, KB, ch), f32),
                pltpu.VMEM((heads, 8, ch), f32),
                pltpu.VMEM((3, d, columns), bf),
                pltpu.VMEM((columns, d), bf),
                pltpu.VMEM((4, ch, d), bf),
                pltpu.VMEM((ch, d), bf),
                pltpu.VMEM((ch, HEAD), f32),
                pltpu.VMEM((ch, HEAD), f32),
                pltpu.VMEM((ch, d), f32),
                pltpu.VMEM((3, 2, ch, d), bf),
                pltpu.VMEM((2, PER, ch // 2, d), bf),
                pltpu.VMEM((4, ch, d), bf),
                pltpu.VMEM((2, ch, d), bf),
                pltpu.SemaphoreType.DMA((4,)),
                pltpu.SemaphoreType.DMA((4,)),
                pltpu.SemaphoreType.DMA((4,)),
                pltpu.SemaphoreType.DMA((4 * PER,)),
                pltpu.SemaphoreType.DMA((4 * PER,)),
                pltpu.SemaphoreType.DMA((4 * PER,)),
                pltpu.SemaphoreType.DMA((4 * PER,)),
            ],
            compiler_params=pltpu.CompilerParams(collective_id=0, has_side_effects=True, vmem_limit_bytes=VMEM),
        )(x, gain, *tables[:2], *tables[2:], wq, wk, wv, wo)
        return y

    tokens, columns = P(("dp", "tp"), None), P(None, "tp")
    return jax.shard_map(
        step,
        mesh=mesh,
        in_specs=(tokens, P(None), columns, columns, columns, P("tp", None)),
        out_specs=tokens,
        check_vma=False,
    )
```
